256 devices in a mesh: owner: 8 (over x, core), rows: 32 (over z, y).
Axes of the slice: x: 4, y: 4, z: 8, core: 2. Of those that a mesh axis runs over, the one named last changes fastest.
Arguments:
- master_gate: float32 [64, 2048, 1408], P('owner', 'rows'), may hold values from -0.25 to 0.25
- master_up: float32 [64, 2048, 1408], P('owner', 'rows'), may hold values from -0.25 to 0.25
- router_weight: float32 [2048, 64], P('rows', 'owner'), may hold values from -0.125 to 0.125
- router_gain: float32 [2048], P('rows'), may hold values from 0.25 to 1.75
Outputs:
- final_gate: bfloat16 [64, 2048, 1408], P('owner', None, 'rows')
- final_up: bfloat16 [64, 2048, 1408], P('owner', None, 'rows')
- scale_gate: float32 [64, 1408], P('owner', 'rows')
- scale_up: float32 [64, 1408], P('owner', 'rows')
- serve_router: bfloat16 [2048, 64], replicated
The draws below stay inside these ranges and needn't reach their ends.
All inputs are finite; a program needn't handle non-finite values. Where the reference program divides by a largest or mean magnitude, that divisor is 1e-20 or more.
Results may differ from the reference program's by a relative error of at most 0.001.
Values may be sent and summed in bfloat16 or wider, within the bound.
A program may use at most 64 MiB of HBM per device.

```python
import jax
import jax.numpy as jnp

EXPERTS = 64
D_MODEL = 2048
D_EXPERT = 1408


def strengthened(entries, key, source, target, blocks, factor):
    owner, partner = [(jnp.arange(entries.shape[dim]) // (entries.shape[dim] // blocks)).reshape([-1 if axis == dim else 1 for axis in range(entries.ndim)]) for dim in (source, target)]
    chosen = jax.random.permutation(key, blocks)[partner]
    strong = (owner == chosen) | (owner == (partner + blocks // 2) % blocks)
    return jnp.where(strong, factor * entries, entries)


def levels(stream_key, dims, pieces, low, largest):
    level = 1.0
    for position, shards_of in pieces:
        steps = jax.random.uniform(jax.random.fold_in(jax.random.fold_in(stream_key, 6), position), (shards_of,), jnp.float32, low / len(pieces), largest / len(pieces))
        level = level * jnp.repeat(jnp.exp(steps), dims[position] // shards_of).reshape((-1,) + (1,) * (len(dims) - 1 - position))
    return level


def centred(rng, extent, spread, limit, shards=(), dtype=jnp.bfloat16):
    result = spread * jax.random.normal(rng, extent, jnp.float32)
    if shards:
        result = result * levels(rng, extent, shards, -0.22, 0.18)
    return jnp.clip(result, -limit, limit).astype(dtype)


def gaussian_with(own_key, shape, scale, bound, cuts, heavy, dtype=jnp.bfloat16):
    drawn = scale * jax.random.normal(own_key, shape, jnp.float32)
    if cuts:
        drawn = drawn * levels(own_key, shape, cuts, -0.22, 0.18)
    return jnp.clip(strengthened(drawn, jax.random.fold_in(own_key, 3), *heavy), -bound, bound).astype(dtype)


def setup_inputs(seed: int = 0) -> dict:
    streams_of = jax.random.split(jax.random.key(seed), 5)
    return {
        "master_gate": gaussian_with(streams_of[0], (EXPERTS, D_MODEL, D_EXPERT), D_MODEL ** -0.5, 0.25, ((0, 8), (1, 32)), (1, 2, 32, 2.75), jnp.float32),
        "master_up": gaussian_with(streams_of[1], (EXPERTS, D_MODEL, D_EXPERT), D_MODEL ** -0.5, 0.25, ((0, 8), (1, 32)), (1, 2, 32, 2.75), jnp.float32),
        "router_weight": centred(streams_of[2], (D_MODEL, EXPERTS), D_MODEL ** -0.5, 0.125, ((0, 32), (1, 8)), jnp.float32),
        "router_gain": jnp.clip(1.0 + 0.15 * jax.random.normal(streams_of[3], (D_MODEL,), jnp.float32), 0.25, 1.75),
    }


def reference(master_gate, master_up, router_weight, router_gain):
    scale_gate = jnp.max(jnp.abs(master_gate), axis=1)
    final_gate = (master_gate / jnp.expand_dims(scale_gate, 1)).astype(jnp.bfloat16)
    scale_up = jnp.max(jnp.abs(master_up), axis=1)
    final_up = (master_up / jnp.expand_dims(scale_up, 1)).astype(jnp.bfloat16)
    serve_router = (router_weight * router_gain[:, None]).astype(jnp.bfloat16)
    return final_gate, final_up, scale_gate, scale_up, serve_router
```

```python
import jax
import jax.numpy as jnp
from jax import lax
from jax.experimental import pallas as pl
from jax.experimental.pallas import tpu as pltpu
from jax.sharding import PartitionSpec as P

MESH = pl.DeviceIdType.MESH
ROWS, OWNERS = 32, 8
E, R, D = 8, 64, 1408
C = D // ROWS
TILES = D // 128
Q = 2 * TILES
MSG = C * E


def owner_of(q):
    return (q * 16) // 11


def remote(src, dst, send, recv, **where):
    return pltpu.make_async_remote_copy(
        src_ref=src, dst_ref=dst, send_sem=send, recv_sem=recv, device_id=where, device_id_type=MESH
    )


def exchange(gate, up, rw, gain, fg, fu, sc_out, sr,
             x, w, xn, ml, parts, sc, rr, s, r, own, rpiece, rparts, rrow, rall,
             in_sem, a_send, a_recv, b_send, b_recv, s_send, s_recv, p_send, p_recv, o_send, o_recv):
    me = lax.axis_index("rows")
    us = lax.axis_index("owner")
    par = lax.rem(me, 2)

    def peer(k):
        return lax.rem(me + k, ROWS)

    loads = []
    for e in range(E):
        for a, ref in enumerate((gate, up)):
            cp = pltpu.make_async_copy(ref.at[e], x.at[a, e], in_sem.at[a, e])
            cp.start()
            loads.append((a, e, cp))
    barrier = pltpu.get_barrier_semaphore()

    def signal_rows(k, _):
        pl.semaphore_signal(barrier, inc=1, device_id={"rows": peer(k)}, device_id_type=MESH)
        return 0

    lax.fori_loop(1, ROWS, signal_rows, 0)

    def signal_owner(k, _):
        pl.semaphore_signal(barrier, inc=1, device_id={"owner": lax.rem(us + k, OWNERS)}, device_id_type=MESH)
        return 0

    lax.fori_loop(1, OWNERS, signal_owner, 0)

    part = rw[...] * gain[...]
    lane64 = lax.broadcasted_iota(jnp.int32, (E, 128), 1) // 64
    rpiece[...] = jnp.where(lane64 == par, jnp.concatenate([part, part], axis=1), 0.0)
    for m in range(8):
        i = lax.broadcasted_iota(jnp.int32, (128, 1024), 0) + m * 128
        k = lax.broadcasted_iota(jnp.int32, (128, 1024), 1)
        hit = (lax.rem(i, 8) == k // 128) & (i // 8 == lax.rem(k, 128))
        w[pl.ds(m * 128, 128), :] = jnp.where(hit, 1.0, 0.0).astype(jnp.bfloat16)
    for a, e, cp in loads:
        cp.wait()
        m = jnp.max(jnp.abs(x[a, e]), axis=0, keepdims=True)
        for t in range(TILES):
            ml[a * TILES + t, pl.ds(e, 1), :] = m[:, t * 128:(t + 1) * 128]

    pl.semaphore_wait(barrier, ROWS - 1 + OWNERS - 1)

    def send_part(q, _):
        to = owner_of(q)

        @pl.when(to != me)
        def _():
            remote(ml.at[q], parts.at[me], a_send.at[q], a_recv.at[me], rows=to).start()

        @pl.when(to == me)
        def _():
            parts[pl.ds(me, 1)] = ml[pl.ds(q, 1)]

        return 0

    lax.fori_loop(0, Q, send_part, 0)

    def send_router(k, _):
        to = peer(k)
        remote(rpiece, rparts.at[me], p_send.at[k], p_recv.at[me], rows=to).start()
        return 0

    lax.fori_loop(1, ROWS, send_router, 0)
    rparts[pl.ds(me, 1)] = rpiece[...][None]

    mine = (11 * me + 15) // 16
    is_owner = owner_of(mine) == me

    @pl.when(is_owner)
    def _():
        def wait_part(k, _):
            src = peer(k)
            remote(ml.at[0], parts.at[src], a_send.at[0], a_recv.at[src], rows=src).wait_recv()
            return 0

        lax.fori_loop(1, ROWS, wait_part, 0)
        sc[pl.ds(mine, 1)] = jnp.max(parts[...], axis=0, keepdims=True)

        def send_scale(k, _):
            remote(sc.at[mine], sc.at[mine], b_send.at[k], b_recv.at[mine], rows=peer(k)).start()
            return 0

        lax.fori_loop(1, ROWS, send_scale, 0)

    def wait_scale(q, _):
        @pl.when(owner_of(q) != me)
        def _():
            remote(sc.at[q], sc.at[q], b_send.at[0], b_recv.at[q], rows=owner_of(q)).wait_recv()

        return 0

    lax.fori_loop(0, Q, wait_scale, 0)
    rr[...] = 1.0 / sc[...]

    for t0 in range(0, TILES, 2):
        n = min(2, TILES - t0)
        for i in range(n):
            t = t0 + i
            for h in range(2):
                a = lax.rem(par + h, 2)
                for e in range(E):
                    v = x[a, e, :, t * 128:(t + 1) * 128] * rr[a * TILES + t, pl.ds(e, 1), :]
                    xn[pl.ds(i * 128 + h * 64, 64), e * 128:(e + 1) * 128] = v.astype(jnp.bfloat16)
        out = lax.dot_general(
            w[...], xn[:n * 128, :], (((1,), (1,)), ((), ())), preferred_element_type=jnp.float32
        )
        for i in range(n):
            s[pl.ds((t0 + i) * 1024, 1024), :] = out[:, i * 128:(i + 1) * 128].astype(jnp.bfloat16)

    def block(j):
        return s.at[pl.ds(pl.multiple_of(j * MSG, 32), MSG)]

    def send_block(k, _):
        to = peer(k)
        remote(block(to), r.at[me], s_send.at[k], s_recv.at[me], rows=to).start()
        return 0

    lax.fori_loop(1, ROWS, send_block, 0)
    keep = pltpu.make_async_copy(block(me), r.at[me], s_recv.at[me])
    keep.start()

    first = (C * me) // 128
    second = jnp.minimum(first + 1, TILES - 1)
    shift = lax.rem(256 - (C * me - 128 * first), 256)
    for a in range(2):
        both = jnp.concatenate([sc[a * TILES + first], sc[a * TILES + second]], axis=1)
        sc_out[a] = pltpu.roll(both, shift, 1)[:, :128]

    def wait_router(k, _):
        src = peer(k)
        remote(rpiece, rparts.at[src], p_send.at[0], p_recv.at[src], rows=src).wait_recv()
        return 0

    lax.fori_loop(1, ROWS, wait_router, 0)
    for p in range(ROWS // 2):
        rrow[:, p * 128:(p + 1) * 128] = rparts[2 * p] + rparts[2 * p + 1]
    for k in range(1, OWNERS):
        to = lax.rem(us + k, OWNERS)
        remote(rrow, rall.at[us], o_send.at[k], o_recv.at[us], owner=to).start()
    rall[pl.ds(us, 1)] = rrow[...][None]

    lane = lax.broadcasted_iota(jnp.int32, (MSG, 128), 1) < 64

    def merge(kk, _):
        p = lax.rem(me // 2 - kk + 16, 16)
        for src in (2 * p, 2 * p + 1):
            pltpu.make_async_copy(r.at[src], r.at[src], s_recv.at[src]).wait()
        even, odd = r[2 * p].astype(jnp.float32), r[2 * p + 1].astype(jnp.float32)
        at = pl.ds(pl.multiple_of(p * 128, 128), 128)
        fg[:, at] = jnp.where(lane, even, odd).astype(jnp.bfloat16)
        fu[:, at] = pltpu.roll(jnp.where(lane, odd, even), 64, 1).astype(jnp.bfloat16)
        return 0

    lax.fori_loop(1, ROWS // 2 + 1, merge, 0)

    for k in range(1, OWNERS):
        src = lax.rem(us + k, OWNERS)
        remote(rrow, rall.at[src], o_send.at[k], o_recv.at[src], owner=src).wait_recv()
    for o in range(OWNERS):
        sr[o * E:(o + 1) * E, :] = rall[o].astype(jnp.bfloat16)

    def drain_a(q, _):
        @pl.when(owner_of(q) != me)
        def _():
            remote(ml.at[q], parts.at[me], a_send.at[q], a_recv.at[me], rows=owner_of(q)).wait_send()

        return 0

    lax.fori_loop(0, Q, drain_a, 0)

    @pl.when(is_owner)
    def _():
        def drain_b(k, _):
            remote(sc.at[mine], sc.at[mine], b_send.at[k], b_recv.at[mine], rows=peer(k)).wait_send()
            return 0

        lax.fori_loop(1, ROWS, drain_b, 0)

    def drain(k, _):
        to = peer(k)
        remote(rpiece, rparts.at[me], p_send.at[k], p_recv.at[me], rows=to).wait_send()
        remote(block(to), r.at[me], s_send.at[k], s_recv.at[me], rows=to).wait_send()
        return 0

    lax.fori_loop(1, ROWS, drain, 0)
    for k in range(1, OWNERS):
        to = lax.rem(us + k, OWNERS)
        remote(rrow, rall.at[us], o_send.at[k], o_recv.at[us], owner=to).wait_send()


def put_out(*refs):
    ins, outs, sem = refs[:5], refs[5:10], refs[10]
    copies = [pltpu.make_async_copy(i, o, sem.at[n]) for n, (i, o) in enumerate(zip(ins, outs))]
    for cp in copies:
        cp.start()
    for cp in copies:
        cp.wait()


def shards(master_gate, master_up, router_weight, router_gain):
    f32, bf16 = jnp.float32, jnp.bfloat16
    vmem, any_ = pl.BlockSpec(memory_space=pltpu.VMEM), pl.BlockSpec(memory_space=pl.ANY)
    dma, scratch = pltpu.SemaphoreType.DMA, pltpu.VMEM
    fg, fu, sc, sr = pl.pallas_call(
        exchange,
        name="exchange",
        out_shape=(
            jax.ShapeDtypeStruct((MSG, ROWS * R), bf16),
            jax.ShapeDtypeStruct((MSG, ROWS * R), bf16),
            jax.ShapeDtypeStruct((2, E, 128), f32),
            jax.ShapeDtypeStruct((OWNERS * E, ROWS * R), bf16),
        ),
        in_specs=[any_, any_, vmem, vmem],
        out_specs=(vmem,) * 4,
        scratch_shapes=[
            scratch((2, E, R, D), f32),
            scratch((1024, 1024), bf16),
            scratch((256, 1024), bf16),
            scratch((Q, E, 128), f32),
            scratch((ROWS, E, 128), f32),
            scratch((Q, E, 128), f32),
            scratch((Q, E, 128), f32),
            scratch((D * E, 128), bf16),
            scratch((ROWS, MSG, 128), bf16),
            scratch((2, E, 128), f32),
            scratch((E, 128), f32),
            scratch((ROWS, E, 128), f32),
            scratch((E, ROWS * R), f32),
            scratch((OWNERS, E, ROWS * R), f32),
            dma((2, E)), dma((Q,)), dma((ROWS,)), dma((ROWS,)), dma((Q,)),
            dma((ROWS,)), dma((ROWS,)), dma((ROWS,)), dma((ROWS,)), dma((OWNERS,)), dma((OWNERS,)),
        ],
        compiler_params=pltpu.CompilerParams(
            collective_id=0, has_side_effects=True, vmem_limit_bytes=40 * 2**20
        ),
    )(master_gate, master_up, router_weight.T, router_gain[None, :])
    sg, su = sc[0, :, :C], sc[1, :, :C]
    fg, fu = fg.reshape(C, E, ROWS * R), fu.reshape(C, E, ROWS * R)
    ins = (fg, fu, sg, su, sr)
    fg, fu, sg, su, sr = pl.pallas_call(
        put_out,
        name="put_out",
        out_shape=tuple(jax.ShapeDtypeStruct(i.shape, i.dtype) for i in ins),
        in_specs=[vmem] * 5,
        out_specs=(any_,) * 5,
        scratch_shapes=[dma((5,))],
    )(*ins)
    return fg.transpose(1, 2, 0), fu.transpose(1, 2, 0), sg, su, sr.T


def solution(mesh):
    return jax.shard_map(
        shards,
        mesh=mesh,
        in_specs=(P("owner", "rows", None), P("owner", "rows", None), P("rows", "owner"), P("rows")),
        out_specs=(
            P("owner", None, "rows"), P("owner", None, "rows"), P("owner", "rows"), P("owner", "rows"), P(),
        ),
        check_vma=False,
    )
```

```python
import jax
import jax.numpy as jnp
from jax import lax
from jax.experimental import pallas as pl
from jax.experimental.pallas import tpu as pltpu
from jax.sharding import PartitionSpec as P

MESH = pl.DeviceIdType.MESH
ROWS, OWNERS = 32, 8
E, R, D = 8, 64, 1408
C = D // ROWS
TILES = D // 128
Q = 2 * TILES
MSG = C * E


def owner_of(q):
    return (q * 16) // 11


def remote(src, dst, send, recv, **where):
    return pltpu.make_async_remote_copy(
        src_ref=src, dst_ref=dst, send_sem=send, recv_sem=recv, device_id=where, device_id_type=MESH
    )


def exchange(gate, up, rw_in, gain_in, fg, fu, sg, su, sr,
             rw, gain, x, w, xn, ml, parts, sc, rr, s, r, own, rpiece, rparts, rrow, rall,
             r_sem, in_sem, a_send, a_recv, b_send, b_recv, s_send, s_recv, p_send, p_recv, o_send, o_recv):
    me = lax.axis_index("rows")
    us = lax.axis_index("owner")
    par = lax.rem(me, 2)

    def peer(k):
        return lax.rem(me + k, ROWS)

    barrier = pltpu.get_barrier_semaphore()

    def signal_rows(k, _):
        pl.semaphore_signal(barrier, inc=1, device_id={"rows": peer(k)}, device_id_type=MESH)
        return 0

    lax.fori_loop(1, ROWS, signal_rows, 0)

    def signal_owner(k, _):
        pl.semaphore_signal(barrier, inc=1, device_id={"owner": lax.rem(us + k, OWNERS)}, device_id_type=MESH)
        return 0

    lax.fori_loop(1, OWNERS, signal_owner, 0)

    loads = []
    for e in range(E):
        for a, ref in enumerate((gate, up)):
            cp = pltpu.make_async_copy(ref.at[e], x.at[a, e], in_sem.at[a, e])
            cp.start()
            loads.append((a, e, cp))
    small = [pltpu.make_async_copy(rw_in, rw, r_sem.at[0]), pltpu.make_async_copy(gain_in, gain, r_sem.at[1])]
    for cp in small:
        cp.start()

    for m in range(8):
        i = lax.broadcasted_iota(jnp.int32, (128, 1024), 0) + m * 128
        k = lax.broadcasted_iota(jnp.int32, (128, 1024), 1)
        hit = (lax.rem(i, 8) == k // 128) & (i // 8 == lax.rem(k, 128))
        w[pl.ds(m * 128, 128), :] = jnp.where(hit, 1.0, 0.0).astype(jnp.bfloat16)
    for cp in small:
        cp.wait()
    part = rw[...] * gain[...]
    lane64 = lax.broadcasted_iota(jnp.int32, (E, 128), 1) // 64
    rpiece[...] = jnp.where(lane64 == par, jnp.concatenate([part, part], axis=1), 0.0)
    for a, e, cp in loads:
        cp.wait()
        m = jnp.max(jnp.abs(x[a, e]), axis=0, keepdims=True)
        for t in range(TILES):
            ml[a * TILES + t, pl.ds(e, 1), :] = m[:, t * 128:(t + 1) * 128]

    pl.semaphore_wait(barrier, ROWS - 1 + OWNERS - 1)

    def send_part(q, _):
        to = owner_of(q)

        @pl.when(to != me)
        def _():
            remote(ml.at[q], parts.at[me], a_send.at[q], a_recv.at[me], rows=to).start()

        @pl.when(to == me)
        def _():
            parts[pl.ds(me, 1)] = ml[pl.ds(q, 1)]

        return 0

    lax.fori_loop(0, Q, send_part, 0)

    def send_router(k, _):
        to = peer(k)
        remote(rpiece, rparts.at[me], p_send.at[k], p_recv.at[me], rows=to).start()
        return 0

    lax.fori_loop(1, ROWS, send_router, 0)
    rparts[pl.ds(me, 1)] = rpiece[...][None]

    mine = (11 * me + 15) // 16
    is_owner = owner_of(mine) == me

    @pl.when(is_owner)
    def _():
        def wait_part(k, _):
            src = peer(k)
            remote(ml.at[0], parts.at[src], a_send.at[0], a_recv.at[src], rows=src).wait_recv()
            return 0

        lax.fori_loop(1, ROWS, wait_part, 0)
        sc[pl.ds(mine, 1)] = jnp.max(parts[...], axis=0, keepdims=True)

        def send_scale(k, _):
            remote(sc.at[mine], sc.at[mine], b_send.at[k], b_recv.at[mine], rows=peer(k)).start()
            return 0

        lax.fori_loop(1, ROWS, send_scale, 0)

    def wait_scale(q, _):
        @pl.when(owner_of(q) != me)
        def _():
            remote(sc.at[q], sc.at[q], b_send.at[0], b_recv.at[q], rows=owner_of(q)).wait_recv()

        return 0

    lax.fori_loop(0, Q, wait_scale, 0)
    rr[...] = 1.0 / sc[...]

    for t0 in range(0, TILES, 2):
        n = min(2, TILES - t0)
        for i in range(n):
            t = t0 + i
            for h in range(2):
                a = lax.rem(par + h, 2)
                for e in range(E):
                    v = x[a, e, :, t * 128:(t + 1) * 128] * rr[a * TILES + t, pl.ds(e, 1), :]
                    xn[pl.ds(i * 128 + h * 64, 64), e * 128:(e + 1) * 128] = v.astype(jnp.bfloat16)
        out = lax.dot_general(
            w[...], xn[:n * 128, :], (((1,), (1,)), ((), ())), preferred_element_type=jnp.float32
        )
        for i in range(n):
            s[pl.ds((t0 + i) * 1024, 1024), :] = out[:, i * 128:(i + 1) * 128].astype(jnp.bfloat16)

    def block(j):
        return s.at[pl.ds(pl.multiple_of(j * MSG, 32), MSG)]

    def send_block(k, _):
        to = peer(k)
        remote(block(to), r.at[me], s_send.at[k], s_recv.at[me], rows=to).start()
        return 0

    lax.fori_loop(1, ROWS, send_block, 0)
    keep = pltpu.make_async_copy(block(me), r.at[me], s_recv.at[me])
    keep.start()

    first = (C * me) // 128
    second = jnp.minimum(first + 1, TILES - 1)
    shift = lax.rem(256 - (C * me - 128 * first), 256)
    for a, ref in enumerate((sg, su)):
        both = jnp.concatenate([sc[a * TILES + first], sc[a * TILES + second]], axis=1)
        ref[...] = pltpu.roll(both, shift, 1)[:, :C]

    def wait_router(k, _):
        src = peer(k)
        remote(rpiece, rparts.at[src], p_send.at[0], p_recv.at[src], rows=src).wait_recv()
        return 0

    lax.fori_loop(1, ROWS, wait_router, 0)
    for p in range(ROWS // 2):
        rrow[:, p * 128:(p + 1) * 128] = rparts[2 * p] + rparts[2 * p + 1]
    for k in range(1, OWNERS):
        to = lax.rem(us + k, OWNERS)
        remote(rrow, rall.at[us], o_send.at[k], o_recv.at[us], owner=to).start()
    rall[pl.ds(us, 1)] = rrow[...][None]

    lane = lax.broadcasted_iota(jnp.int32, (MSG, 128), 1) < 64

    def merge(kk, _):
        p = lax.rem(me // 2 - kk + 16, 16)
        for src in (2 * p, 2 * p + 1):
            pltpu.make_async_copy(r.at[src], r.at[src], s_recv.at[src]).wait()
        even, odd = r[2 * p].astype(jnp.float32), r[2 * p + 1].astype(jnp.float32)
        at = pl.ds(pl.multiple_of(p * 128, 128), 128)
        fg[:, at] = jnp.where(lane, even, odd).astype(jnp.bfloat16)
        fu[:, at] = pltpu.roll(jnp.where(lane, odd, even), 64, 1).astype(jnp.bfloat16)
        return 0

    lax.fori_loop(1, 13, merge, 0)
    for k in range(1, OWNERS):
        src = lax.rem(us + k, OWNERS)
        remote(rrow, rall.at[src], o_send.at[k], o_recv.at[src], owner=src).wait_recv()
    for o in range(OWNERS):
        sr[o * E:(o + 1) * E, :] = rall[o].astype(jnp.bfloat16)
    lax.fori_loop(13, ROWS // 2 + 1, merge, 0)

    def drain_a(q, _):
        @pl.when(owner_of(q) != me)
        def _():
            remote(ml.at[q], parts.at[me], a_send.at[q], a_recv.at[me], rows=owner_of(q)).wait_send()

        return 0

    lax.fori_loop(0, Q, drain_a, 0)

    @pl.when(is_owner)
    def _():
        def drain_b(k, _):
            remote(sc.at[mine], sc.at[mine], b_send.at[k], b_recv.at[mine], rows=peer(k)).wait_send()
            return 0

        lax.fori_loop(1, ROWS, drain_b, 0)

    def drain(k, _):
        to = peer(k)
        remote(rpiece, rparts.at[me], p_send.at[k], p_recv.at[me], rows=to).wait_send()
        remote(block(to), r.at[me], s_send.at[k], s_recv.at[me], rows=to).wait_send()
        return 0

    lax.fori_loop(1, ROWS, drain, 0)
    for k in range(1, OWNERS):
        to = lax.rem(us + k, OWNERS)
        remote(rrow, rall.at[us], o_send.at[k], o_recv.at[us], owner=to).wait_send()


def put_out(*refs):
    ins, outs, sem = refs[:5], refs[5:10], refs[10]
    copies = [pltpu.make_async_copy(i, o, sem.at[n]) for n, (i, o) in enumerate(zip(ins, outs))]
    for cp in copies:
        cp.start()
    for cp in copies:
        cp.wait()


def shards(master_gate, master_up, router_weight, router_gain):
    f32, bf16 = jnp.float32, jnp.bfloat16
    vmem, any_, hbm = (pl.BlockSpec(memory_space=m) for m in (pltpu.VMEM, pl.ANY, pltpu.HBM))
    dma, scratch = pltpu.SemaphoreType.DMA, pltpu.VMEM
    fg, fu, sg, su, sr = pl.pallas_call(
        exchange,
        name="exchange",
        out_shape=(
            jax.ShapeDtypeStruct((MSG, ROWS * R), bf16),
            jax.ShapeDtypeStruct((MSG, ROWS * R), bf16),
            jax.ShapeDtypeStruct((E, C), f32),
            jax.ShapeDtypeStruct((E, C), f32),
            jax.ShapeDtypeStruct((OWNERS * E, ROWS * R), bf16),
        ),
        in_specs=[hbm] * 4,
        out_specs=(vmem,) * 5,
        scratch_shapes=[
            scratch((E, R), f32),
            scratch((1, R), f32),
            scratch((2, E, R, D), f32),
            scratch((1024, 1024), bf16),
            scratch((256, 1024), bf16),
            scratch((Q, E, 128), f32),
            scratch((ROWS, E, 128), f32),
            scratch((Q, E, 128), f32),
            scratch((Q, E, 128), f32),
            scratch((D * E, 128), bf16),
            scratch((ROWS, MSG, 128), bf16),
            scratch((2, E, 128), f32),
            scratch((E, 128), f32),
            scratch((ROWS, E, 128), f32),
            scratch((E, ROWS * R), f32),
            scratch((OWNERS, E, ROWS * R), f32),
            dma((2,)), dma((2, E)), dma((Q,)), dma((ROWS,)), dma((ROWS,)), dma((Q,)),
            dma((ROWS,)), dma((ROWS,)), dma((ROWS,)), dma((ROWS,)), dma((OWNERS,)), dma((OWNERS,)),
        ],
        compiler_params=pltpu.CompilerParams(
            collective_id=0, has_side_effects=True, vmem_limit_bytes=40 * 2**20
        ),
    )(*(pltpu.with_memory_space_constraint(v, pltpu.HBM) for v in (master_gate, master_up, router_weight.T, router_gain[None, :])))
    fg, fu = fg.reshape(C, E, ROWS * R), fu.reshape(C, E, ROWS * R)
    ins = (fg, fu, sg, su, sr)
    fg, fu, sg, su, sr = pl.pallas_call(
        put_out,
        name="put_out",
        out_shape=tuple(jax.ShapeDtypeStruct(i.shape, i.dtype) for i in ins),
        in_specs=[any_] * 5,
        out_specs=(hbm,) * 5,
        scratch_shapes=[dma((5,))],
        compiler_params=pltpu.CompilerParams(vmem_limit_bytes=2**20),
    )(*ins)
    return fg.transpose(1, 2, 0), fu.transpose(1, 2, 0), sg, su, sr.T


def solution(mesh):
    return jax.shard_map(
        shards,
        mesh=mesh,
        in_specs=(P("owner", "rows", None), P("owner", "rows", None), P("rows", "owner"), P("rows")),
        out_specs=(
            P("owner", None, "rows"), P("owner", None, "rows"), P("owner", "rows"), P("owner", "rows"), P(),
        ),
        check_vma=False,
    )
```

```python
import jax
import jax.numpy as jnp
from jax import lax
from jax.experimental import pallas as pl
from jax.experimental.pallas import tpu as pltpu
from jax.sharding import PartitionSpec as P

MESH = pl.DeviceIdType.MESH
ROWS, OWNERS = 32, 8
E, R, D = 8, 64, 1408
C = D // ROWS
TILES = D // 128
Q = 2 * TILES
MSG = C * E


def owner_of(q):
    return (ROWS * lax.rem(q, TILES)) // TILES + q // TILES


def remote(src, dst, send, recv, **where):
    return pltpu.make_async_remote_copy(
        src_ref=src, dst_ref=dst, send_sem=send, recv_sem=recv, device_id=where, device_id_type=MESH
    )


def exchange(gate, up, rw_in, gain_in, fg, fu, sg, su, sr,
             rw, gain, x, w, xn, ml, parts, sc, rr, s, r, own, rpiece, rparts, rrow, rall,
             r_sem, in_sem, a_send, a_recv, b_send, b_recv, s_send, s_recv, p_send, p_recv, o_send, o_recv):
    me = lax.axis_index("rows")
    us = lax.axis_index("owner")
    par = lax.rem(me, 2)

    def peer(k):
        return lax.rem(me + k, ROWS)

    barrier = pltpu.get_barrier_semaphore()

    def signal_rows(k, _):
        pl.semaphore_signal(barrier, inc=1, device_id={"rows": peer(k)}, device_id_type=MESH)
        return 0

    lax.fori_loop(1, ROWS, signal_rows, 0)

    def signal_owner(k, _):
        pl.semaphore_signal(barrier, inc=1, device_id={"owner": lax.rem(us + k, OWNERS)}, device_id_type=MESH)
        return 0

    lax.fori_loop(1, OWNERS, signal_owner, 0)

    loads = []
    for e in range(E):
        for a, ref in enumerate((gate, up)):
            cp = pltpu.make_async_copy(ref.at[e], x.at[a, e], in_sem.at[a, e])
            cp.start()
            loads.append((a, e, cp))
    small = [pltpu.make_async_copy(rw_in, rw, r_sem.at[0]), pltpu.make_async_copy(gain_in, gain, r_sem.at[1])]
    for cp in small:
        cp.start()

    for cp in small:
        cp.wait()
    part = rw[...] * gain[...]
    lane64 = lax.broadcasted_iota(jnp.int32, (E, 128), 1) // 64
    rpiece[...] = jnp.where(lane64 == par, jnp.concatenate([part, part], axis=1), 0.0)
    for a, e, cp in loads:
        cp.wait()
        m = jnp.max(jnp.abs(x[a, e]), axis=0, keepdims=True)
        for t in range(TILES):
            ml[a * TILES + t, pl.ds(e, 1), :] = m[:, t * 128:(t + 1) * 128]

    pl.semaphore_wait(barrier, ROWS - 1 + OWNERS - 1)

    def send_part(q, _):
        to = owner_of(q)

        @pl.when(to != me)
        def _():
            remote(ml.at[q], parts.at[me], a_send.at[q], a_recv.at[me], rows=to).start()

        @pl.when(to == me)
        def _():
            parts[pl.ds(me, 1)] = ml[pl.ds(q, 1)]

        return 0

    lax.fori_loop(0, Q, send_part, 0)

    def send_router(k, _):
        to = peer(k)
        remote(rpiece, rparts.at[me], p_send.at[k], p_recv.at[me], rows=to).start()
        return 0

    lax.fori_loop(1, ROWS, send_router, 0)
    rparts[pl.ds(me, 1)] = rpiece[...][None]

    for m in range(8):
        i = lax.broadcasted_iota(jnp.int32, (128, 1024), 0) + m * 128
        k = lax.broadcasted_iota(jnp.int32, (128, 1024), 1)
        hit = (lax.rem(i, 8) == k // 128) & (i // 8 == lax.rem(k, 128))
        w[pl.ds(m * 128, 128), :] = jnp.where(hit, 1.0, 0.0).astype(jnp.bfloat16)
    gate_tile, up_tile = (TILES * me + ROWS - 1) // ROWS, (TILES * (me - 1) + ROWS - 1) // ROWS
    owns_gate = (ROWS * gate_tile) // TILES == me
    owns_up = (me > 0) & ((ROWS * up_tile) // TILES == me - 1)
    is_owner = (owns_gate & (gate_tile < TILES)) | owns_up
    mine = jnp.where(owns_up, TILES + up_tile, gate_tile)

    @pl.when(is_owner)
    def _():
        def wait_part(k, _):
            src = peer(k)
            remote(ml.at[0], parts.at[src], a_send.at[0], a_recv.at[src], rows=src).wait_recv()
            return 0

        lax.fori_loop(1, ROWS, wait_part, 0)
        sc[pl.ds(mine, 1)] = jnp.max(parts[...], axis=0, keepdims=True)

        def send_scale(k, _):
            remote(sc.at[mine], sc.at[mine], b_send.at[k], b_recv.at[mine], rows=peer(k)).start()
            return 0

        lax.fori_loop(1, ROWS, send_scale, 0)

    def wait_scale(q, _):
        @pl.when(owner_of(q) != me)
        def _():
            remote(sc.at[q], sc.at[q], b_send.at[0], b_recv.at[q], rows=owner_of(q)).wait_recv()

        return 0

    def tile_scales(t):
        for q in (t, TILES + t):
            wait_scale(q, 0)
            rr[pl.ds(q, 1)] = 1.0 / sc[pl.ds(q, 1)]

    def block(j):
        return s.at[pl.ds(pl.multiple_of(j * MSG, 32), MSG)]

    def send_block(k, _):
        to = peer(k)
        remote(block(to), r.at[me], s_send.at[k], s_recv.at[me], rows=to).start()
        return 0

    def send_block_down(k, _):
        return send_block(ROWS - k, _)

    right, left = C * (me + 1), C * (me + ROWS)
    right_tile, left_tile = right // 128, (left - 1) // 128
    right_sent, left_sent = 0, 0
    for step in range(6):
        tiles = (lax.rem(right_tile + step, TILES), lax.rem(left_tile - step, TILES))
        tile_scales(tiles[0])
        pl.when(tiles[0] != tiles[1])(lambda t=tiles[1]: tile_scales(t))
        for i, t in enumerate(tiles):
            lanes = pl.ds(pl.multiple_of(t * 128, 128), 128)
            for h in range(2):
                a = lax.rem(par + h, 2)
                for e in range(E):
                    v = x[a, e, :, lanes] * rr[a * TILES + t, pl.ds(e, 1), :]
                    xn[i * 128 + h * 64:i * 128 + (h + 1) * 64, e * 128:(e + 1) * 128] = v.astype(jnp.bfloat16)
        out = lax.dot_general(
            w[...], xn[...], (((1,), (1,)), ((), ())), preferred_element_type=jnp.float32
        )
        for i, t in enumerate(tiles):
            at = pl.ds(pl.multiple_of(t * 1024, 1024), 1024)
            s[at, :] = out[:, i * 128:(i + 1) * 128].astype(jnp.bfloat16)
        if step < 5:
            right_done = (128 * (right_tile + step + 1) - right) // C
            left_done = (left - 128 * (left_tile - step)) // C
        else:
            right_done, left_done = ROWS // 2, ROWS // 2 - 1
        lax.fori_loop(right_sent + 1, right_done + 1, send_block, 0)
        lax.fori_loop(left_sent + 1, left_done + 1, send_block_down, 0)
        right_sent, left_sent = right_done, left_done

    keep = pltpu.make_async_copy(block(me), r.at[me], s_recv.at[me])
    keep.start()

    first = (C * me) // 128
    second = jnp.minimum(first + 1, TILES - 1)
    shift = lax.rem(256 - (C * me - 128 * first), 256)
    for a, ref in enumerate((sg, su)):
        both = jnp.concatenate([sc[a * TILES + first], sc[a * TILES + second]], axis=1)
        ref[...] = pltpu.roll(both, shift, 1)[:, :C]

    def wait_router(k, _):
        src = peer(k)
        remote(rpiece, rparts.at[src], p_send.at[0], p_recv.at[src], rows=src).wait_recv()
        return 0

    lax.fori_loop(1, ROWS, wait_router, 0)
    for p in range(ROWS // 2):
        rrow[:, p * 128:(p + 1) * 128] = rparts[2 * p] + rparts[2 * p + 1]
    for k in range(1, OWNERS):
        to = lax.rem(us + k, OWNERS)
        remote(rrow, rall.at[us], o_send.at[k], o_recv.at[us], owner=to).start()
    rall[pl.ds(us, 1)] = rrow[...][None]

    lane = lax.broadcasted_iota(jnp.int32, (MSG, 128), 1) < 64

    def merge(kk, _):
        p = lax.rem(me // 2 + 16 + lax.rem(kk, 2) * ((kk + 1) // 2) - (1 - lax.rem(kk, 2)) * (kk // 2), 16)
        for src in (2 * p, 2 * p + 1):
            pltpu.make_async_copy(r.at[src], r.at[src], s_recv.at[src]).wait()
        even, odd = r[2 * p].astype(jnp.float32), r[2 * p + 1].astype(jnp.float32)
        at = pl.ds(pl.multiple_of(p * 128, 128), 128)
        fg[:, at] = jnp.where(lane, even, odd).astype(jnp.bfloat16)
        fu[:, at] = pltpu.roll(jnp.where(lane, odd, even), 64, 1).astype(jnp.bfloat16)
        return 0

    lax.fori_loop(0, 12, merge, 0)
    for k in range(1, OWNERS):
        src = lax.rem(us + k, OWNERS)
        remote(rrow, rall.at[src], o_send.at[k], o_recv.at[src], owner=src).wait_recv()
    for o in range(OWNERS):
        sr[o * E:(o + 1) * E, :] = rall[o].astype(jnp.bfloat16)
    lax.fori_loop(12, ROWS // 2, merge, 0)

    def drain_a(q, _):
        @pl.when(owner_of(q) != me)
        def _():
            remote(ml.at[q], parts.at[me], a_send.at[q], a_recv.at[me], rows=owner_of(q)).wait_send()

        return 0

    lax.fori_loop(0, Q, drain_a, 0)

    @pl.when(is_owner)
    def _():
        def drain_b(k, _):
            remote(sc.at[mine], sc.at[mine], b_send.at[k], b_recv.at[mine], rows=peer(k)).wait_send()
            return 0

        lax.fori_loop(1, ROWS, drain_b, 0)

    def drain(k, _):
        to = peer(k)
        remote(rpiece, rparts.at[me], p_send.at[k], p_recv.at[me], rows=to).wait_send()
        remote(block(to), r.at[me], s_send.at[k], s_recv.at[me], rows=to).wait_send()
        return 0

    lax.fori_loop(1, ROWS, drain, 0)
    for k in range(1, OWNERS):
        to = lax.rem(us + k, OWNERS)
        remote(rrow, rall.at[us], o_send.at[k], o_recv.at[us], owner=to).wait_send()


def put_out(*refs):
    ins, outs, sem = refs[:5], refs[5:10], refs[10]
    copies = [pltpu.make_async_copy(i, o, sem.at[n]) for n, (i, o) in enumerate(zip(ins, outs))]
    for cp in copies:
        cp.start()
    for cp in copies:
        cp.wait()


def shards(master_gate, master_up, router_weight, router_gain):
    f32, bf16 = jnp.float32, jnp.bfloat16
    vmem, any_, hbm = (pl.BlockSpec(memory_space=m) for m in (pltpu.VMEM, pl.ANY, pltpu.HBM))
    dma, scratch = pltpu.SemaphoreType.DMA, pltpu.VMEM
    fg, fu, sg, su, sr = pl.pallas_call(
        exchange,
        name="exchange",
        out_shape=(
            jax.ShapeDtypeStruct((MSG, ROWS * R), bf16),
            jax.ShapeDtypeStruct((MSG, ROWS * R), bf16),
            jax.ShapeDtypeStruct((E, C), f32),
            jax.ShapeDtypeStruct((E, C), f32),
            jax.ShapeDtypeStruct((OWNERS * E, ROWS * R), bf16),
        ),
        in_specs=[hbm] * 4,
        out_specs=(vmem,) * 5,
        scratch_shapes=[
            scratch((E, R), f32),
            scratch((1, R), f32),
            scratch((2, E, R, D), f32),
            scratch((1024, 1024), bf16),
            scratch((256, 1024), bf16),
            scratch((Q, E, 128), f32),
            scratch((ROWS, E, 128), f32),
            scratch((Q, E, 128), f32),
            scratch((Q, E, 128), f32),
            scratch((D * E, 128), bf16),
            scratch((ROWS, MSG, 128), bf16),
            scratch((2, E, 128), f32),
            scratch((E, 128), f32),
            scratch((ROWS, E, 128), f32),
            scratch((E, ROWS * R), f32),
            scratch((OWNERS, E, ROWS * R), f32),
            dma((2,)), dma((2, E)), dma((Q,)), dma((ROWS,)), dma((ROWS,)), dma((Q,)),
            dma((ROWS,)), dma((ROWS,)), dma((ROWS,)), dma((ROWS,)), dma((OWNERS,)), dma((OWNERS,)),
        ],
        compiler_params=pltpu.CompilerParams(
            collective_id=0, has_side_effects=True, vmem_limit_bytes=40 * 2**20
        ),
    )(*(pltpu.with_memory_space_constraint(v, pltpu.HBM) for v in (master_gate, master_up, router_weight.T, router_gain[None, :])))
    fg, fu = fg.reshape(C, E, ROWS * R), fu.reshape(C, E, ROWS * R)
    ins = (fg, fu, sg, su, sr)
    fg, fu, sg, su, sr = pl.pallas_call(
        put_out,
        name="put_out",
        out_shape=tuple(jax.ShapeDtypeStruct(i.shape, i.dtype) for i in ins),
        in_specs=[any_] * 5,
        out_specs=(hbm,) * 5,
        scratch_shapes=[dma((5,))],
        compiler_params=pltpu.CompilerParams(vmem_limit_bytes=2**20),
    )(*ins)
    return fg.transpose(1, 2, 0), fu.transpose(1, 2, 0), sg, su, sr.T


def solution(mesh):
    return jax.shard_map(
        shards,
        mesh=mesh,
        in_specs=(P("owner", "rows", None), P("owner", "rows", None), P("rows", "owner"), P("rows")),
        out_specs=(
            P("owner", None, "rows"), P("owner", None, "rows"), P("owner", "rows"), P("owner", "rows"), P(),
        ),
        check_vma=False,
    )
```

```python
import jax
import jax.numpy as jnp
from jax import lax
from jax.experimental import pallas as pl
from jax.experimental.pallas import tpu as pltpu
from jax.sharding import PartitionSpec as P

MESH = pl.DeviceIdType.MESH
ROWS, OWNERS = 32, 8
E, R, D = 8, 64, 1408
C = D // ROWS
TILES = D // 128
Q = 2 * TILES
MSG = C * E
START = 2


def owner_of(q):
    return (ROWS * lax.rem(q, TILES)) // TILES + q // TILES


def remote(src, dst, send, recv, **where):
    return pltpu.make_async_remote_copy(
        src_ref=src, dst_ref=dst, send_sem=send, recv_sem=recv, device_id=where, device_id_type=MESH
    )


def exchange(gate, up, rw_in, gain_in, fg, fu, sg, su, sr,
             rw, gain, x, w, xn, ml, parts, sc, rr, s, r, own, rpiece, rparts, rrow, rall,
             r_sem, in_sem, a_send, a_recv, b_send, b_recv, s_send, s_recv, p_send, p_recv, o_send, o_recv):
    me = lax.axis_index("rows")
    us = lax.axis_index("owner")
    par = lax.rem(me, 2)

    def peer(k):
        return lax.rem(me + k, ROWS)

    def far(k):
        return ROWS // 2 + lax.rem(k, 2) * (k // 2) - (1 - lax.rem(k, 2)) * (k // 2)

    loads = []
    for e in range(E):
        for a, ref in enumerate((gate, up)):
            cp = pltpu.make_async_copy(ref.at[e], x.at[a, e], in_sem.at[a, e])
            cp.start()
            loads.append((a, e, cp))
    barrier = pltpu.get_barrier_semaphore()

    def signal_rows(k, _):
        pl.semaphore_signal(barrier, inc=1, device_id={"rows": peer(far(k))}, device_id_type=MESH)
        return 0

    lax.fori_loop(1, ROWS, signal_rows, 0)

    def signal_owner(k, _):
        pl.semaphore_signal(barrier, inc=1, device_id={"owner": lax.rem(us + k, OWNERS)}, device_id_type=MESH)
        return 0

    lax.fori_loop(1, OWNERS, signal_owner, 0)

    small = [pltpu.make_async_copy(rw_in, rw, r_sem.at[0]), pltpu.make_async_copy(gain_in, gain, r_sem.at[1])]
    for cp in small:
        cp.start()

    for cp in small:
        cp.wait()
    part = rw[...] * gain[...]
    lane64 = lax.broadcasted_iota(jnp.int32, (E, 128), 1) // 64
    rpiece[...] = jnp.where(lane64 == par, jnp.concatenate([part, part], axis=1), 0.0)
    for a, e, cp in loads:
        cp.wait()
        m = jnp.max(jnp.abs(x[a, e]), axis=0, keepdims=True)
        for t in range(TILES):
            ml[a * TILES + t, pl.ds(e, 1), :] = m[:, t * 128:(t + 1) * 128]

    pl.semaphore_wait(barrier, ROWS - 1 + OWNERS - 1)

    def owned(d):
        gate_tile, up_tile = (TILES * d + ROWS - 1) // ROWS, (TILES * (d - 1) + ROWS - 1) // ROWS
        owns_up = (d > 0) & ((ROWS * up_tile) // TILES == d - 1)
        owns_gate = (gate_tile < TILES) & ((ROWS * gate_tile) // TILES == d)
        return owns_gate | owns_up, jnp.where(owns_up, TILES + up_tile, jnp.minimum(gate_tile, TILES - 1))

    is_owner, mine = owned(me)

    def send_part(k, _):
        to = peer(far(k))
        wanted, q = owned(to)

        @pl.when(wanted)
        def _():
            remote(ml.at[q], parts.at[me], a_send.at[q], a_recv.at[me], rows=to).start()

        return 0

    lax.fori_loop(1, ROWS, send_part, 0)
    parts[pl.ds(me, 1)] = ml[pl.ds(mine, 1)]

    def send_router(k, _):
        to = peer(k)
        remote(rpiece, rparts.at[me], p_send.at[k], p_recv.at[me], rows=to).start()
        return 0

    lax.fori_loop(1, ROWS, send_router, 0)
    rparts[pl.ds(me, 1)] = rpiece[...][None]

    for m in range(8):
        i = lax.broadcasted_iota(jnp.int32, (128, 1024), 0) + m * 128
        k = lax.broadcasted_iota(jnp.int32, (128, 1024), 1)
        hit = (lax.rem(i, 8) == k // 128) & (i // 8 == lax.rem(k, 128))
        w[pl.ds(m * 128, 128), :] = jnp.where(hit, 1.0, 0.0).astype(jnp.bfloat16)
    @pl.when(is_owner)
    def _():
        def wait_part(k, _):
            src = peer(k)
            remote(ml.at[0], parts.at[src], a_send.at[0], a_recv.at[src], rows=src).wait_recv()
            return 0

        lax.fori_loop(1, ROWS, wait_part, 0)
        sc[pl.ds(mine, 1)] = jnp.max(parts[...], axis=0, keepdims=True)

        def send_scale(k, _):
            remote(sc.at[mine], sc.at[mine], b_send.at[k], b_recv.at[mine], rows=peer(far(k))).start()
            return 0

        lax.fori_loop(1, ROWS, send_scale, 0)

    def wait_scale(q, _):
        @pl.when(owner_of(q) != me)
        def _():
            remote(sc.at[q], sc.at[q], b_send.at[0], b_recv.at[q], rows=owner_of(q)).wait_recv()

        return 0

    def tile_scales(t):
        for q in (t, TILES + t):
            wait_scale(q, 0)
            rr[pl.ds(q, 1)] = 1.0 / sc[pl.ds(q, 1)]

    def block(j):
        return s.at[pl.ds(pl.multiple_of(j * MSG, 32), MSG)]

    def send_block(k, _):
        to = peer(k)
        remote(block(to), r.at[me], s_send.at[k], s_recv.at[me], rows=to).start()
        return 0

    def send_block_down(k, _):
        return send_block(ROWS - k, _)

    right, left = C * (me + 1), C * (me + ROWS)
    right_tile, left_tile = right // 128, (left - 1) // 128

    def first(step):
        if step == 0:
            return 0, 0
        return (
            (128 * (right_tile + step) - right + C - 1) // C,
            (left - 128 * (left_tile - step + 1) + C - 1) // C,
        )

    right_sent, left_sent = first(START)
    for step in (*range(START, 6), *range(START - 1, -1, -1)):
        tiles = (lax.rem(right_tile + step, TILES), lax.rem(left_tile - step, TILES))
        tile_scales(tiles[0])
        pl.when(tiles[0] != tiles[1])(lambda t=tiles[1]: tile_scales(t))
        for i, t in enumerate(tiles):
            lanes = pl.ds(pl.multiple_of(t * 128, 128), 128)
            for h in range(2):
                a = lax.rem(par + h, 2)
                for e in range(E):
                    v = x[a, e, :, lanes] * rr[a * TILES + t, pl.ds(e, 1), :]
                    xn[i * 128 + h * 64:i * 128 + (h + 1) * 64, e * 128:(e + 1) * 128] = v.astype(jnp.bfloat16)
        out = lax.dot_general(
            w[...], xn[...], (((1,), (1,)), ((), ())), preferred_element_type=jnp.float32
        )
        for i, t in enumerate(tiles):
            at = pl.ds(pl.multiple_of(t * 1024, 1024), 1024)
            s[at, :] = out[:, i * 128:(i + 1) * 128].astype(jnp.bfloat16)
        if step < START:
            (right_sent, left_sent), (right_done, left_done) = first(step), first(step + 1)
        elif step == 5:
            right_done, left_done = ROWS // 2, ROWS // 2 - 1
        else:
            right_done = (128 * (right_tile + step + 1) - right) // C
            left_done = (left - 128 * (left_tile - step)) // C
        lax.fori_loop(right_sent + 1, right_done + 1, send_block, 0)
        lax.fori_loop(left_sent + 1, left_done + 1, send_block_down, 0)
        right_sent, left_sent = right_done, left_done

    keep = pltpu.make_async_copy(block(me), r.at[me], s_recv.at[me])
    keep.start()

    first = (C * me) // 128
    second = jnp.minimum(first + 1, TILES - 1)
    shift = lax.rem(256 - (C * me - 128 * first), 256)
    for a, ref in enumerate((sg, su)):
        both = jnp.concatenate([sc[a * TILES + first], sc[a * TILES + second]], axis=1)
        ref[...] = pltpu.roll(both, shift, 1)[:, :C]

    def wait_router(k, _):
        src = peer(k)
        remote(rpiece, rparts.at[src], p_send.at[0], p_recv.at[src], rows=src).wait_recv()
        return 0

    lax.fori_loop(1, ROWS, wait_router, 0)
    for p in range(ROWS // 2):
        rrow[:, p * 128:(p + 1) * 128] = rparts[2 * p] + rparts[2 * p + 1]
    for k in range(1, OWNERS):
        to = lax.rem(us + k, OWNERS)
        remote(rrow, rall.at[us], o_send.at[k], o_recv.at[us], owner=to).start()
    rall[pl.ds(us, 1)] = rrow[...][None]

    lane = lax.broadcasted_iota(jnp.int32, (MSG, 128), 1) < 64

    def merge(kk, _):
        p = lax.rem(me // 2 + 16 + lax.rem(kk, 2) * ((kk + 1) // 2) - (1 - lax.rem(kk, 2)) * (kk // 2), 16)
        for src in (2 * p, 2 * p + 1):
            pltpu.make_async_copy(r.at[src], r.at[src], s_recv.at[src]).wait()
        even, odd = r[2 * p].astype(jnp.float32), r[2 * p + 1].astype(jnp.float32)
        at = pl.ds(pl.multiple_of(p * 128, 128), 128)
        fg[:, at] = jnp.where(lane, even, odd).astype(jnp.bfloat16)
        fu[:, at] = pltpu.roll(jnp.where(lane, odd, even), 64, 1).astype(jnp.bfloat16)
        return 0

    lax.fori_loop(0, 12, merge, 0)
    for k in range(1, OWNERS):
        src = lax.rem(us + k, OWNERS)
        remote(rrow, rall.at[src], o_send.at[k], o_recv.at[src], owner=src).wait_recv()
    for o in range(OWNERS):
        sr[o * E:(o + 1) * E, :] = rall[o].astype(jnp.bfloat16)
    lax.fori_loop(12, ROWS // 2, merge, 0)

    def drain_a(q, _):
        @pl.when(owner_of(q) != me)
        def _():
            remote(ml.at[q], parts.at[me], a_send.at[q], a_recv.at[me], rows=owner_of(q)).wait_send()

        return 0

    lax.fori_loop(0, Q, drain_a, 0)

    @pl.when(is_owner)
    def _():
        def drain_b(k, _):
            remote(sc.at[mine], sc.at[mine], b_send.at[k], b_recv.at[mine], rows=peer(far(k))).wait_send()
            return 0

        lax.fori_loop(1, ROWS, drain_b, 0)

    def drain(k, _):
        to = peer(k)
        remote(rpiece, rparts.at[me], p_send.at[k], p_recv.at[me], rows=to).wait_send()
        remote(block(to), r.at[me], s_send.at[k], s_recv.at[me], rows=to).wait_send()
        return 0

    lax.fori_loop(1, ROWS, drain, 0)
    for k in range(1, OWNERS):
        to = lax.rem(us + k, OWNERS)
        remote(rrow, rall.at[us], o_send.at[k], o_recv.at[us], owner=to).wait_send()


def put_out(*refs):
    ins, outs, sem = refs[:5], refs[5:10], refs[10]
    pieces = [(i, o) for i, o in zip(ins[2:], outs[2:])]
    for i, o in zip(ins[:2], outs[:2]):
        pieces += [(i.at[pl.ds(c, C // 4)], o.at[pl.ds(c, C // 4)]) for c in range(0, C, C // 4)]
    copies = [pltpu.make_async_copy(i, o, sem.at[n]) for n, (i, o) in enumerate(pieces)]
    for cp in copies:
        cp.start()
    for cp in copies:
        cp.wait()


def shards(master_gate, master_up, router_weight, router_gain):
    f32, bf16 = jnp.float32, jnp.bfloat16
    vmem, any_, hbm = (pl.BlockSpec(memory_space=m) for m in (pltpu.VMEM, pl.ANY, pltpu.HBM))
    dma, scratch = pltpu.SemaphoreType.DMA, pltpu.VMEM
    fg, fu, sg, su, sr = pl.pallas_call(
        exchange,
        name="exchange",
        out_shape=(
            jax.ShapeDtypeStruct((MSG, ROWS * R), bf16),
            jax.ShapeDtypeStruct((MSG, ROWS * R), bf16),
            jax.ShapeDtypeStruct((E, C), f32),
            jax.ShapeDtypeStruct((E, C), f32),
            jax.ShapeDtypeStruct((OWNERS * E, ROWS * R), bf16),
        ),
        in_specs=[hbm] * 4,
        out_specs=(vmem,) * 5,
        scratch_shapes=[
            scratch((E, R), f32),
            scratch((1, R), f32),
            scratch((2, E, R, D), f32),
            scratch((1024, 1024), bf16),
            scratch((256, 1024), bf16),
            scratch((Q, E, 128), f32),
            scratch((ROWS, E, 128), f32),
            scratch((Q, E, 128), f32),
            scratch((Q, E, 128), f32),
            scratch((D * E, 128), bf16),
            scratch((ROWS, MSG, 128), bf16),
            scratch((2, E, 128), f32),
            scratch((E, 128), f32),
            scratch((ROWS, E, 128), f32),
            scratch((E, ROWS * R), f32),
            scratch((OWNERS, E, ROWS * R), f32),
            dma((2,)), dma((2, E)), dma((Q,)), dma((ROWS,)), dma((ROWS,)), dma((Q,)),
            dma((ROWS,)), dma((ROWS,)), dma((ROWS,)), dma((ROWS,)), dma((OWNERS,)), dma((OWNERS,)),
        ],
        compiler_params=pltpu.CompilerParams(
            collective_id=0, has_side_effects=True, vmem_limit_bytes=40 * 2**20
        ),
    )(*(pltpu.with_memory_space_constraint(v, pltpu.HBM) for v in (master_gate, master_up, router_weight.T, router_gain[None, :])))
    fg, fu = fg.reshape(C, E, ROWS * R), fu.reshape(C, E, ROWS * R)
    ins = (fg, fu, sg, su, sr)
    fg, fu, sg, su, sr = pl.pallas_call(
        put_out,
        name="put_out",
        out_shape=tuple(jax.ShapeDtypeStruct(i.shape, i.dtype) for i in ins),
        in_specs=[any_] * 5,
        out_specs=(hbm,) * 5,
        scratch_shapes=[dma((11,))],
        compiler_params=pltpu.CompilerParams(vmem_limit_bytes=2**20),
    )(*ins)
    return fg.transpose(1, 2, 0), fu.transpose(1, 2, 0), sg, su, sr.T


def solution(mesh):
    return jax.shard_map(
        shards,
        mesh=mesh,
        in_specs=(P("owner", "rows", None), P("owner", "rows", None), P("rows", "owner"), P("rows")),
        out_specs=(
            P("owner", None, "rows"), P("owner", None, "rows"), P("owner", "rows"), P("owner", "rows"), P(),
        ),
        check_vma=False,
    )
```

```python
import jax
import jax.numpy as jnp
from jax import lax
from jax.experimental import pallas as pl
from jax.experimental.pallas import tpu as pltpu
from jax.sharding import PartitionSpec as P

MESH = pl.DeviceIdType.MESH
ROWS, OWNERS = 32, 8
E, R, D = 8, 64, 1408
C = D // ROWS
TILES = D // 128
Q = 2 * TILES
MSG = C * E
START = 2


def owner_of(q):
    return (ROWS * lax.rem(q, TILES)) // TILES + q // TILES


def remote(src, dst, send, recv, **where):
    return pltpu.make_async_remote_copy(
        src_ref=src, dst_ref=dst, send_sem=send, recv_sem=recv, device_id=where, device_id_type=MESH
    )


def exchange(gate, up, rw_in, gain_in, fg, fu, sg, su, sr,
             rw, gain, x, w, xn, ml, parts, sc, rr, s, r, own, rpiece, rparts, rrow, rall,
             r_sem, in_sem, a_send, a_recv, b_send, b_recv, s_send, s_recv, p_send, p_recv, o_send, o_recv):
    me = lax.axis_index("rows")
    us = lax.axis_index("owner")
    par = lax.rem(me, 2)

    def peer(k):
        return lax.rem(me + k, ROWS)

    def far(k):
        return ROWS // 2 + lax.rem(k, 2) * (k // 2) - (1 - lax.rem(k, 2)) * (k // 2)

    loads = []
    for e in range(E):
        for a, ref in enumerate((gate, up)):
            cp = pltpu.make_async_copy(ref.at[e], x.at[a, e], in_sem.at[a, e])
            cp.start()
            loads.append((a, e, cp))
    barrier = pltpu.get_barrier_semaphore()

    def signal_rows(k, _):
        pl.semaphore_signal(barrier, inc=1, device_id={"rows": peer(far(k))}, device_id_type=MESH)
        return 0

    lax.fori_loop(1, ROWS, signal_rows, 0)

    def signal_owner(k, _):
        pl.semaphore_signal(barrier, inc=1, device_id={"owner": lax.rem(us + k, OWNERS)}, device_id_type=MESH)
        return 0

    lax.fori_loop(1, OWNERS, signal_owner, 0)

    small = [pltpu.make_async_copy(rw_in, rw, r_sem.at[0]), pltpu.make_async_copy(gain_in, gain, r_sem.at[1])]
    for cp in small:
        cp.start()

    for cp in small:
        cp.wait()
    part = rw[...] * gain[...]
    lane64 = lax.broadcasted_iota(jnp.int32, (E, 128), 1) // 64
    rpiece[...] = jnp.where(lane64 == par, jnp.concatenate([part, part], axis=1), 0.0)
    for a, e, cp in loads:
        cp.wait()
        m = jnp.max(jnp.abs(x[a, e]), axis=0, keepdims=True)
        for t in range(TILES):
            ml[a * TILES + t, pl.ds(e, 1), :] = m[:, t * 128:(t + 1) * 128]

    pl.semaphore_wait(barrier, ROWS - 1 + OWNERS - 1)

    def owned(d):
        gate_tile, up_tile = (TILES * d + ROWS - 1) // ROWS, (TILES * (d - 1) + ROWS - 1) // ROWS
        owns_up = (d > 0) & ((ROWS * up_tile) // TILES == d - 1)
        owns_gate = (gate_tile < TILES) & ((ROWS * gate_tile) // TILES == d)
        return owns_gate | owns_up, jnp.where(owns_up, TILES + up_tile, jnp.minimum(gate_tile, TILES - 1))

    is_owner, mine = owned(me)

    def send_part(k, _):
        to = peer(far(k))
        wanted, q = owned(to)

        @pl.when(wanted)
        def _():
            remote(ml.at[q], parts.at[me], a_send.at[q], a_recv.at[me], rows=to).start()

        return 0

    lax.fori_loop(1, ROWS, send_part, 0)
    parts[pl.ds(me, 1)] = ml[pl.ds(mine, 1)]

    def send_router(k, _):
        to = peer(k)
        remote(rpiece, rparts.at[me], p_send.at[k], p_recv.at[me], rows=to).start()
        return 0

    lax.fori_loop(1, ROWS, send_router, 0)
    rparts[pl.ds(me, 1)] = rpiece[...][None]

    for m in range(8):
        i = lax.broadcasted_iota(jnp.int32, (128, 1024), 0) + m * 128
        k = lax.broadcasted_iota(jnp.int32, (128, 1024), 1)
        hit = (lax.rem(i, 8) == k // 128) & (i // 8 == lax.rem(k, 128))
        w[pl.ds(m * 128, 128), :] = jnp.where(hit, 1.0, 0.0).astype(jnp.bfloat16)
    @pl.when(is_owner)
    def _():
        def wait_part(k, _):
            src = peer(k)
            remote(ml.at[0], parts.at[src], a_send.at[0], a_recv.at[src], rows=src).wait_recv()
            return 0

        lax.fori_loop(1, ROWS, wait_part, 0)
        sc[pl.ds(mine, 1)] = jnp.max(parts[...], axis=0, keepdims=True)

        def send_scale(k, _):
            remote(sc.at[mine], sc.at[mine], b_send.at[k], b_recv.at[mine], rows=peer(far(k))).start()
            return 0

        lax.fori_loop(1, ROWS, send_scale, 0)

    def wait_scale(q, _):
        @pl.when(owner_of(q) != me)
        def _():
            remote(sc.at[q], sc.at[q], b_send.at[0], b_recv.at[q], rows=owner_of(q)).wait_recv()

        return 0

    def tile_scales(t):
        for q in (t, TILES + t):
            wait_scale(q, 0)
            rr[pl.ds(q, 1)] = 1.0 / sc[pl.ds(q, 1)]

    def block(j):
        return s.at[pl.ds(pl.multiple_of(j * MSG, 32), MSG)]

    def send_block(k, _):
        to = peer(k)
        remote(block(to), r.at[me], s_send.at[k], s_recv.at[me], rows=to).start()
        return 0

    def send_block_down(k, _):
        return send_block(ROWS - k, _)

    right, left = C * (me + 1), C * (me + ROWS)
    right_tile, left_tile = right // 128, (left - 1) // 128

    def first(step):
        if step == 0:
            return 0, 0
        return (
            (128 * (right_tile + step) - right + C - 1) // C,
            (left - 128 * (left_tile - step + 1) + C - 1) // C,
        )

    right_sent, left_sent = first(START)
    for step in (*range(START, 6), *range(START - 1, -1, -1)):
        tiles = (lax.rem(right_tile + step, TILES), lax.rem(left_tile - step, TILES))
        tile_scales(tiles[0])
        pl.when(tiles[0] != tiles[1])(lambda t=tiles[1]: tile_scales(t))
        for i, t in enumerate(tiles):
            lanes = pl.ds(pl.multiple_of(t * 128, 128), 128)
            for h in range(2):
                a = lax.rem(par + h, 2)
                for e in range(E):
                    v = x[a, e, :, lanes] * rr[a * TILES + t, pl.ds(e, 1), :]
                    xn[i * 128 + h * 64:i * 128 + (h + 1) * 64, e * 128:(e + 1) * 128] = v.astype(jnp.bfloat16)
        out = lax.dot_general(
            w[...], xn[...], (((1,), (1,)), ((), ())), preferred_element_type=jnp.float32
        )
        for i, t in enumerate(tiles):
            at = pl.ds(pl.multiple_of(t * 1024, 1024), 1024)
            s[at, :] = out[:, i * 128:(i + 1) * 128].astype(jnp.bfloat16)
        if step < START:
            (right_sent, left_sent), (right_done, left_done) = first(step), first(step + 1)
        elif step == 5:
            right_done, left_done = ROWS // 2, ROWS // 2 - 1
        else:
            right_done = (128 * (right_tile + step + 1) - right) // C
            left_done = (left - 128 * (left_tile - step)) // C
        lax.fori_loop(right_sent + 1, right_done + 1, send_block, 0)
        lax.fori_loop(left_sent + 1, left_done + 1, send_block_down, 0)
        right_sent, left_sent = right_done, left_done

    keep = pltpu.make_async_copy(block(me), r.at[me], s_recv.at[me])
    keep.start()

    first = (C * me) // 128
    second = jnp.minimum(first + 1, TILES - 1)
    shift = lax.rem(256 - (C * me - 128 * first), 256)
    for a, ref in enumerate((sg, su)):
        both = jnp.concatenate([sc[a * TILES + first], sc[a * TILES + second]], axis=1)
        ref[...] = pltpu.roll(both, shift, 1)[:, :C]

    def wait_router(k, _):
        src = peer(k)
        remote(rpiece, rparts.at[src], p_send.at[0], p_recv.at[src], rows=src).wait_recv()
        return 0

    lax.fori_loop(1, ROWS, wait_router, 0)
    for p in range(ROWS // 2):
        rrow[:, p * 128:(p + 1) * 128] = rparts[2 * p] + rparts[2 * p + 1]
    for k in range(1, OWNERS):
        to = lax.rem(us + k, OWNERS)
        remote(rrow, rall.at[us], o_send.at[k], o_recv.at[us], owner=to).start()
    rall[pl.ds(us, 1)] = rrow[...][None]

    def drain_a(q, _):
        @pl.when(owner_of(q) != me)
        def _():
            remote(ml.at[q], parts.at[me], a_send.at[q], a_recv.at[me], rows=owner_of(q)).wait_send()

        return 0

    lax.fori_loop(0, Q, drain_a, 0)

    @pl.when(is_owner)
    def _():
        def drain_b(k, _):
            remote(sc.at[mine], sc.at[mine], b_send.at[k], b_recv.at[mine], rows=peer(far(k))).wait_send()
            return 0

        lax.fori_loop(1, ROWS, drain_b, 0)

    def drain_router(k, _):
        remote(rpiece, rparts.at[me], p_send.at[k], p_recv.at[me], rows=peer(k)).wait_send()
        return 0

    lax.fori_loop(1, ROWS, drain_router, 0)

    lane = lax.broadcasted_iota(jnp.int32, (MSG, 128), 1) < 64

    def merge(n, _):
        kk = jnp.where(n < 11, n + 5, 15 - n)
        p = lax.rem(me // 2 + 16 + lax.rem(kk, 2) * ((kk + 1) // 2) - (1 - lax.rem(kk, 2)) * (kk // 2), 16)
        for src in (2 * p, 2 * p + 1):
            pltpu.make_async_copy(r.at[src], r.at[src], s_recv.at[src]).wait()
        even, odd = r[2 * p].astype(jnp.float32), r[2 * p + 1].astype(jnp.float32)
        at = pl.ds(pl.multiple_of(p * 128, 128), 128)
        fg[:, at] = jnp.where(lane, even, odd).astype(jnp.bfloat16)
        fu[:, at] = pltpu.roll(jnp.where(lane, odd, even), 64, 1).astype(jnp.bfloat16)
        return 0

    lax.fori_loop(0, 12, merge, 0)
    for k in range(1, OWNERS):
        src = lax.rem(us + k, OWNERS)
        remote(rrow, rall.at[src], o_send.at[k], o_recv.at[src], owner=src).wait_recv()
    for o in range(OWNERS):
        sr[o * E:(o + 1) * E, :] = rall[o].astype(jnp.bfloat16)
    for k in range(1, OWNERS):
        to = lax.rem(us + k, OWNERS)
        remote(rrow, rall.at[us], o_send.at[k], o_recv.at[us], owner=to).wait_send()
    lax.fori_loop(12, ROWS // 2, merge, 0)

    def drain(k, _):
        to = peer(k)
        remote(block(to), r.at[me], s_send.at[k], s_recv.at[me], rows=to).wait_send()
        return 0

    lax.fori_loop(1, ROWS, drain, 0)


def put_out(*refs):
    ins, outs, sem = refs[:5], refs[5:10], refs[10]
    pieces = [(i, o) for i, o in zip(ins[2:], outs[2:])]
    for i, o in zip(ins[:2], outs[:2]):
        pieces += [(i.at[pl.ds(c, C // 4)], o.at[pl.ds(c, C // 4)]) for c in range(0, C, C // 4)]
    copies = [pltpu.make_async_copy(i, o, sem.at[n]) for n, (i, o) in enumerate(pieces)]
    for cp in copies:
        cp.start()
    for cp in copies:
        cp.wait()


def shards(master_gate, master_up, router_weight, router_gain):
    f32, bf16 = jnp.float32, jnp.bfloat16
    vmem, any_, hbm = (pl.BlockSpec(memory_space=m) for m in (pltpu.VMEM, pl.ANY, pltpu.HBM))
    dma, scratch = pltpu.SemaphoreType.DMA, pltpu.VMEM
    fg, fu, sg, su, sr = pl.pallas_call(
        exchange,
        name="exchange",
        out_shape=(
            jax.ShapeDtypeStruct((MSG, ROWS * R), bf16),
            jax.ShapeDtypeStruct((MSG, ROWS * R), bf16),
            jax.ShapeDtypeStruct((E, C), f32),
            jax.ShapeDtypeStruct((E, C), f32),
            jax.ShapeDtypeStruct((OWNERS * E, ROWS * R), bf16),
        ),
        in_specs=[hbm] * 4,
        out_specs=(vmem,) * 5,
        scratch_shapes=[
            scratch((E, R), f32),
            scratch((1, R), f32),
            scratch((2, E, R, D), f32),
            scratch((1024, 1024), bf16),
            scratch((256, 1024), bf16),
            scratch((Q, E, 128), f32),
            scratch((ROWS, E, 128), f32),
            scratch((Q, E, 128), f32),
            scratch((Q, E, 128), f32),
            scratch((D * E, 128), bf16),
            scratch((ROWS, MSG, 128), bf16),
            scratch((2, E, 128), f32),
            scratch((E, 128), f32),
            scratch((ROWS, E, 128), f32),
            scratch((E, ROWS * R), f32),
            scratch((OWNERS, E, ROWS * R), f32),
            dma((2,)), dma((2, E)), dma((Q,)), dma((ROWS,)), dma((ROWS,)), dma((Q,)),
            dma((ROWS,)), dma((ROWS,)), dma((ROWS,)), dma((ROWS,)), dma((OWNERS,)), dma((OWNERS,)),
        ],
        compiler_params=pltpu.CompilerParams(
            collective_id=0, has_side_effects=True, vmem_limit_bytes=40 * 2**20
        ),
    )(*(pltpu.with_memory_space_constraint(v, pltpu.HBM) for v in (master_gate, master_up, router_weight.T, router_gain[None, :])))
    fg, fu = fg.reshape(C, E, ROWS * R), fu.reshape(C, E, ROWS * R)
    ins = (fg, fu, sg, su, sr)
    fg, fu, sg, su, sr = pl.pallas_call(
        put_out,
        name="put_out",
        out_shape=tuple(jax.ShapeDtypeStruct(i.shape, i.dtype) for i in ins),
        in_specs=[any_] * 5,
        out_specs=(hbm,) * 5,
        scratch_shapes=[dma((11,))],
        compiler_params=pltpu.CompilerParams(vmem_limit_bytes=2**20),
    )(*ins)
    return fg.transpose(1, 2, 0), fu.transpose(1, 2, 0), sg, su, sr.T


def solution(mesh):
    return jax.shard_map(
        shards,
        mesh=mesh,
        in_specs=(P("owner", "rows", None), P("owner", "rows", None), P("rows", "owner"), P("rows")),
        out_specs=(
            P("owner", None, "rows"), P("owner", None, "rows"), P("owner", "rows"), P("owner", "rows"), P(),
        ),
        check_vma=False,
    )
```
